32 devices in a mesh: dp: 16 (over z, x, core), seq: 2 (over y).
Axes of the slice: x: 2, y: 2, z: 4, core: 2. Of those that a mesh axis runs over, the one named last changes fastest.
Arguments:
- queries: bfloat16 [4096, 6144], P(('dp', 'seq')), may hold values from -8 to 8
- latent: bfloat16 [4096, 512], P(('dp', 'seq')), may hold values from -6 to 6
- key_rope: bfloat16 [4096, 64], P(('dp', 'seq')), may hold values from -8 to 8
- up_weight: bfloat16 [512, 8192], P(None, 'seq'), may hold values from -0.25 to 0.25
- out_grad: bfloat16 [4096, 4096], P(('dp', 'seq')), may hold values from -6 to 6
Outputs:
- latent_grad: float32 [4096, 512], P(('dp', 'seq'))
- weight_grad: float32 [512, 8192], P('dp', 'seq')
The draws below stay inside these ranges and needn't reach their ends.
All inputs are finite; a program needn't handle non-finite values.
Results may differ from the reference program's by a relative error of at most 0.0065.
Values may be sent and summed in bfloat16 or wider, within the bound.
A program may use at most 64 MiB of HBM per device.

```python
import jax
import jax.numpy as jnp
from jax import lax

KV_RANK = 512
H = 32
NOPE = 128
ROPE = 64
VDIM = 128
LENGTH = 256
TOKENS = 4096
N_DP = 16


def joint_draw(key):
    base_key = jax.random.fold_in(key, 7)
    query_key, rope_key = jax.random.split(base_key, 2)
    query_width = NOPE + ROPE
    queries = jnp.clip(jax.random.normal(query_key, (TOKENS, H * query_width), jnp.float32), -4.0, 4.0)
    rope = jnp.clip(jax.random.normal(rope_key, (TOKENS, ROPE), jnp.float32), -4.0, 4.0)
    return (queries, rope)


def draw_queries(key, part):
    return joint_draw(key)[0].astype(jnp.bfloat16)


def draw_key_rope(key, part):
    return joint_draw(key)[1].astype(jnp.bfloat16)


def raised(drawn, stream_key, source, target, blocks, factor):
    owner, partner = [(jnp.arange(drawn.shape[dim]) // (drawn.shape[dim] // blocks)).reshape([-1 if axis == dim else 1 for axis in range(drawn.ndim)]) for dim in (source, target)]
    chosen = jax.random.permutation(stream_key, blocks)[partner]
    strong = (owner == chosen) | (owner == (partner + blocks // 2) % blocks)
    return jnp.where(strong, factor * drawn, drawn)


def shard_levels(own_key, shape, shards, low, top_value):
    factor_of, own = 1.0, jax.random.fold_in(own_key, 6)
    for dim, blocks in shards:
        draws = jnp.exp(jax.random.uniform(jax.random.fold_in(own, dim), (blocks,), jnp.float32, low / len(shards), top_value / len(shards)))
        factor_of = factor_of * jnp.repeat(draws, shape[dim] // blocks).reshape([-1 if axis == dim else 1 for axis in range(len(shape))])
    return factor_of


def gaussian(stream_key, extent, width, most, cuts=(), dtype=jnp.bfloat16):
    level = shard_levels(stream_key, extent, cuts, -0.22, 0.18) if cuts else 1.0
    drawn = jax.random.normal(stream_key, extent, jnp.float32) * width * level
    return jnp.minimum(jnp.maximum(drawn, -most), most).astype(dtype)


def gaussian_with(key, extent, deviation, reach, shards, heavy, kind=jnp.bfloat16):
    entries = deviation * jax.random.normal(key, extent, jnp.float32)
    if shards:
        entries = entries * shard_levels(key, extent, shards, -0.22, 0.18)
    return jnp.clip(raised(entries, jax.random.fold_in(key, 3), *heavy), -reach, reach).astype(kind)


def setup_inputs(seed: int = 0) -> dict:
    streams_of = jax.random.split(jax.random.key(seed), 6)
    return {
        "queries": draw_queries(jax.random.fold_in(streams_of[5], 71), 0),
        "latent": gaussian_with(streams_of[1], (TOKENS, KV_RANK), 1.0, 6.0, ((0, 32),), (0, 1, 32, 2.75)),
        "key_rope": draw_key_rope(jax.random.fold_in(streams_of[5], 71), 0),
        "up_weight": gaussian(streams_of[3], (KV_RANK, H * (NOPE + VDIM)), KV_RANK ** -0.5, 0.25, ((1, 2),)),
        "out_grad": gaussian(streams_of[4], (TOKENS, H * VDIM), 1.0, 6.0, ((0, 32),)),
    }


def head_grads(query_head, kv_head, grad_head, rope_seq):
    score_scale = (NOPE + ROPE) ** -0.5
    query_nope = query_head[:, :NOPE]
    query_rope = query_head[:, NOPE:]
    keys_nope = kv_head[:, :NOPE]
    values = kv_head[:, NOPE:]
    scores = jnp.dot(query_nope, keys_nope.T, preferred_element_type=jnp.float32)
    scores = scores + jnp.dot(query_rope, rope_seq.T, preferred_element_type=jnp.float32)
    scores = scores * score_scale
    query_pos = lax.broadcasted_iota(jnp.int32, (LENGTH, LENGTH), 0)
    key_pos = lax.broadcasted_iota(jnp.int32, (LENGTH, LENGTH), 1)
    scores = jnp.where(key_pos <= query_pos, scores, jnp.float32(-1e30))
    row_max = jnp.max(scores, axis=1, keepdims=True)
    expo = jnp.exp(scores - row_max)
    probs = expo / jnp.sum(expo, axis=1, keepdims=True)
    probs_rounded = probs.astype(jnp.bfloat16)
    value_grad = jnp.dot(probs_rounded.T, grad_head, preferred_element_type=jnp.float32)
    prob_grad = jnp.dot(grad_head, values.T, preferred_element_type=jnp.float32)
    row_dot = jnp.sum(probs * prob_grad, axis=1, keepdims=True)
    score_grad = (probs * (prob_grad - row_dot) * score_scale).astype(jnp.bfloat16)
    key_grad = jnp.dot(score_grad.T, query_nope, preferred_element_type=jnp.float32)
    return jnp.concatenate([key_grad, value_grad], axis=1).astype(jnp.bfloat16)


def reference(queries, latent, key_rope, up_weight, out_grad):
    query_width = NOPE + ROPE
    kv_width = NOPE + VDIM

    def one_sequence(total, inputs):
        latent_seq, rope_seq, query_seq, grad_seq = inputs
        kv_cols = jnp.dot(latent_seq, up_weight, preferred_element_type=jnp.float32).astype(jnp.bfloat16)
        stacked = (query_seq.reshape(LENGTH, H, query_width).transpose(1, 0, 2),
                   kv_cols.reshape(LENGTH, H, kv_width).transpose(1, 0, 2),
                   grad_seq.reshape(LENGTH, H, VDIM).transpose(1, 0, 2))
        head_cols = lax.map(lambda parts: head_grads(parts[0], parts[1], parts[2], rope_seq), stacked)
        grad_cols = head_cols.transpose(1, 0, 2).reshape(LENGTH, H * kv_width)
        latent_seq_grad = jnp.dot(grad_cols, up_weight.T, preferred_element_type=jnp.float32)
        total = total + jnp.dot(latent_seq.T, grad_cols, preferred_element_type=jnp.float32)
        return total, latent_seq_grad

    inputs = (latent.reshape(N_DP, LENGTH, KV_RANK), key_rope.reshape(N_DP, LENGTH, ROPE),
              queries.reshape(N_DP, LENGTH, H * query_width), out_grad.reshape(N_DP, LENGTH, H * VDIM))
    start_total = jnp.zeros((KV_RANK, H * kv_width), jnp.float32)
    total, latent_parts = lax.scan(one_sequence, start_total, inputs)
    return latent_parts.reshape(TOKENS, KV_RANK), total / N_DP
```

```python
import functools
import math

import jax
import jax.numpy as jnp
from jax import lax
from jax.experimental import pallas as pl
from jax.experimental.pallas import tpu as pltpu
from jax.sharding import PartitionSpec as P

NOPE = 128
ROPE = 64
VDIM = 128
QW = NOPE + ROPE
KVW = NOPE + VDIM
PAIR_Q = 2 * QW
PAIR_G = 2 * VDIM
PAIR_KV = 2 * KVW
AHEAD = 4
MESH = pl.DeviceIdType.MESH
F32 = jnp.float32
BF16 = jnp.bfloat16
NT = (((1,), (1,)), ((), ()))


def kernel(
    n_seq, na, nb, pairs,
    q_hbm, lat_hbm, rope_hbm, w_hbm, g_hbm,
    lg_ref, wg_ref,
    qbuf, gbuf, wbuf, latbuf, ropebuf, lat_t, rope_l, rope_r, gc, lg_acc,
    part, dsend, drecv, keepx, xsend, xrecv, keepz, zsend, zrecv, lsend, lrecv,
    q_local, g_local, w_local, lat_local, rope_local,
    q_send, q_recv, g_send, g_recv, lat_send, lat_recv, rope_send, rope_recv,
    d_send, d_recv, x_send, x_recv, z_send, z_recv, l_send, l_recv,
):
    seq = lax.axis_index("seq")
    dp = lax.axis_index("dp")
    core = lax.rem(dp, 2)
    chip = dp // 2
    a_me = chip // nb
    b_me = lax.rem(chip, nb)
    n_chips = na * nb
    rows = lat_hbm.shape[0]
    length = n_seq * rows
    rank = lat_hbm.shape[1]
    block = rank // (2 * n_chips)
    scale = QW ** -0.5

    def seq_to(o):
        return lax.rem(seq + o, n_seq)

    def chip_core(a, b, c):
        return (a * nb + b) * 2 + c

    core_partner = chip_core(a_me, b_me, 1 - core)

    barrier = pltpu.get_barrier_semaphore()
    greeted = 0
    for o in range(1, n_seq):
        pl.semaphore_signal(barrier, inc=1, device_id={"seq": seq_to(o)}, device_id_type=MESH)
        greeted += 1
    pl.semaphore_signal(barrier, inc=1, device_id={"dp": core_partner}, device_id_type=MESH)
    greeted += 1
    for o in range(1, nb):
        pl.semaphore_signal(
            barrier, inc=1, device_id={"dp": chip_core(a_me, lax.rem(b_me + o, nb), core)},
            device_id_type=MESH,
        )
        greeted += 1
    for o in range(1, na):
        pl.semaphore_signal(
            barrier, inc=1, device_id={"dp": chip_core(lax.rem(a_me + o, na), b_me, core)},
            device_id_type=MESH,
        )
        greeted += 1

    def columns(owner, p, width):
        return pl.ds(pl.multiple_of((owner * pairs + p) * width, 128), width)

    def local_q(p):
        return pltpu.make_async_copy(
            q_hbm.at[:, columns(seq, p, PAIR_Q)], qbuf.at[p, seq], q_local.at[p]
        )

    def local_g(p):
        return pltpu.make_async_copy(
            g_hbm.at[:, columns(seq, p, PAIR_G)], gbuf.at[p, seq], g_local.at[p]
        )

    def local_w(p):
        return pltpu.make_async_copy(
            w_hbm.at[:, pl.ds(pl.multiple_of(p * PAIR_KV, 128), PAIR_KV)],
            wbuf.at[p], w_local.at[p],
        )

    local_lat = pltpu.make_async_copy(lat_hbm, latbuf.at[seq], lat_local)
    local_rope = pltpu.make_async_copy(rope_hbm, ropebuf.at[seq], rope_local)

    def remote(src, dst, send, recv, device):
        return pltpu.make_async_remote_copy(
            src_ref=src, dst_ref=dst, send_sem=send, recv_sem=recv,
            device_id=device, device_id_type=MESH,
        )

    def send_lat(o):
        return remote(lat_hbm, latbuf.at[seq], lat_send.at[o], lat_recv.at[o], {"seq": seq_to(o)})

    def send_rope(o):
        return remote(
            rope_hbm, ropebuf.at[seq], rope_send.at[o], rope_recv.at[o], {"seq": seq_to(o)}
        )

    def send_q(p, o):
        return remote(
            q_hbm.at[:, columns(seq_to(o), p, PAIR_Q)], qbuf.at[p, seq],
            q_send.at[p, o], q_recv.at[p, o], {"seq": seq_to(o)},
        )

    def send_g(p, o):
        return remote(
            g_hbm.at[:, columns(seq_to(o), p, PAIR_G)], gbuf.at[p, seq],
            g_send.at[p, o], g_recv.at[p, o], {"seq": seq_to(o)},
        )

    def send_d(p):
        return remote(dsend.at[p], drecv.at[p], d_send.at[p], d_recv.at[p], {"dp": core_partner})

    def send_x(p, o):
        return remote(
            xsend.at[p, o - 1], xrecv.at[p, o - 1], x_send.at[p, o - 1], x_recv.at[p, o - 1],
            {"dp": chip_core(a_me, lax.rem(b_me + o, nb), core)},
        )

    def send_z(p, o):
        return remote(
            zsend.at[p, o - 1], zrecv.at[p, o - 1], z_send.at[p, o - 1], z_recv.at[p, o - 1],
            {"dp": chip_core(lax.rem(a_me + o, na), b_me, core)},
        )

    def send_l(o):
        return remote(
            lsend.at[o - 1], lrecv.at[o - 1], l_send.at[o - 1], l_recv.at[o - 1],
            {"seq": seq_to(o)},
        )

    local_lat.start()
    local_rope.start()

    @pl.loop(0, pairs)
    def _(p):
        local_w(p).start()
        local_q(p).start()
        local_g(p).start()

    pl.semaphore_wait(barrier, greeted)

    for o in range(1, n_seq):
        send_lat(o).start()
        send_rope(o).start()

    def start_sends(p):
        for o in range(1, n_seq):
            send_q(p, o).start()
            send_g(p, o).start()

    @pl.loop(0, min(AHEAD, pairs))
    def _(p):
        start_sends(p)

    local_lat.wait()
    local_rope.wait()
    for o in range(1, n_seq):
        send_lat(o).wait_recv()
        send_rope(o).wait_recv()

    for s in range(n_seq):
        lat_t[:, s * rows:(s + 1) * rows] = latbuf[s].T
        rope = ropebuf[s]
        from_lane = lax.broadcasted_iota(jnp.int32, (ROPE, 128), 0)
        to_lane = lax.broadcasted_iota(jnp.int32, (ROPE, 128), 1)
        low = (from_lane == to_lane).astype(F32).astype(BF16)
        high = (from_lane + (128 - ROPE) == to_lane).astype(F32).astype(BF16)
        rope_l[s * rows:(s + 1) * rows] = jnp.dot(rope, low, preferred_element_type=F32)
        rope_r[s * rows:(s + 1) * rows] = jnp.dot(rope, high, preferred_element_type=F32)
    lg_acc[...] = jnp.zeros_like(lg_acc)

    span = math.gcd(length, 256)
    n_blocks = length // span
    lane = lax.broadcasted_iota(jnp.int32, (length, 128), 1)
    lower = lane < 64

    def head(keys, values, q_all, g_all):
        key_parts = [None] * n_blocks
        value_parts = [None] * n_blocks
        for b in range(n_blocks):
            end = (b + 1) * span
            q = q_all[b * span:end]
            g = g_all[b * span:end]
            scores = lax.dot_general(keys[:end], q, NT, preferred_element_type=F32) * scale
            key_pos = lax.broadcasted_iota(jnp.int32, (end, span), 0)
            query_pos = b * span + lax.broadcasted_iota(jnp.int32, (end, span), 1)
            scores = jnp.where(key_pos <= query_pos, scores, F32(-1e30))
            top = jnp.max(scores, axis=0, keepdims=True)
            expo = jnp.exp(scores - top)
            probs = expo * (1.0 / jnp.sum(expo, axis=0, keepdims=True))
            value_part = jnp.dot(probs.astype(BF16), g, preferred_element_type=F32)
            prob_grad = lax.dot_general(values[:end], g, NT, preferred_element_type=F32)
            row_dot = jnp.sum(probs * prob_grad, axis=0, keepdims=True)
            score_grad = (probs * (prob_grad - row_dot) * scale).astype(BF16)
            key_part = jnp.dot(score_grad, q, preferred_element_type=F32)
            for k in range(b + 1):
                at = slice(k * span, (k + 1) * span)
                if key_parts[k] is None:
                    key_parts[k], value_parts[k] = key_part[at], value_part[at]
                else:
                    key_parts[k] = key_parts[k] + key_part[at]
                    value_parts[k] = value_parts[k] + value_part[at]
        if n_blocks == 1:
            return key_parts[0], value_parts[0]
        return jnp.concatenate(key_parts, axis=0), jnp.concatenate(value_parts, axis=0)

    def compute(p):
        lat = latbuf[...].reshape(length, rank)
        local_w(p).wait()
        kv = jnp.dot(lat, wbuf[p], preferred_element_type=F32)
        keys0 = jnp.concatenate([kv[:, :128], rope_l[...]], axis=1).astype(BF16)
        turned = pltpu.roll(kv[:, 256:384], 64, 1)
        keys1 = jnp.concatenate(
            [jnp.where(lower, 0.0, turned), jnp.where(lower, turned, rope_r[...])], axis=1
        ).astype(BF16)
        local_q(p).wait()
        local_g(p).wait()
        for o in range(1, n_seq):
            send_q(p, o).wait_recv()
            send_g(p, o).wait_recv()
        q_all = qbuf[p].reshape(length, PAIR_Q)
        g_all = gbuf[p].reshape(length, PAIR_G)
        kg0, vg0 = head(keys0, kv[:, 128:256].astype(BF16), q_all[:, :256], g_all[:, :128])
        gc[:, 0:128] = kg0[:, :128].astype(BF16)
        gc[:, 128:256] = vg0.astype(BF16)
        kg1, vg1 = head(keys1, kv[:, 384:512].astype(BF16), q_all[:, 128:384], g_all[:, 128:])
        kg1 = jnp.where(lower, pltpu.roll(kg1[:, :128], 64, 1), pltpu.roll(kg1[:, 128:], 64, 1))
        gc[:, 256:384] = kg1.astype(BF16)
        gc[:, 384:512] = vg1.astype(BF16)
        grads = gc[...]
        slot = lax.rem(p, 2)
        product = jnp.dot(lat_t[...], grads, preferred_element_type=F32)
        for d in range(2 * n_chips):
            part[slot, d] = product[d * block:(d + 1) * block]
        for k in range(n_chips):
            dsend[p, k] = part[slot, 2 * k + 1 - core].astype(BF16)
        send_d(p).start()
        lg_acc[...] += lax.dot_general(grads, wbuf[p], NT, preferred_element_type=F32)

    def stage_x(p):
        slot = lax.rem(p, 2)
        send_d(p).wait_recv()

        def chip_sum(k):
            return part[slot, 2 * k + core] + drecv[p, k].astype(F32)

        for o in range(1, nb):
            b = lax.rem(b_me + o, nb)
            for a in range(na):
                xsend[p, o - 1, a] = chip_sum(a * nb + b).astype(BF16)
            send_x(p, o).start()
        for a in range(na):
            keepx[slot, a] = chip_sum(a * nb + b_me)

    def stage_z(p):
        slot = lax.rem(p, 2)
        for o in range(1, nb):
            send_x(p, o).wait_recv()

        def total(a):
            out = keepx[slot, a]
            for o in range(1, nb):
                out = out + xrecv[p, o - 1, a].astype(F32)
            return out

        for o in range(1, na):
            zsend[p, o - 1] = total(lax.rem(a_me + o, na)).astype(BF16)
            send_z(p, o).start()
        keepz[slot] = total(a_me)

    def stage_out(p):
        slot = lax.rem(p, 2)
        out = keepz[slot]
        for o in range(1, na):
            send_z(p, o).wait_recv()
            out = out + zrecv[p, o - 1].astype(F32)
        at = pl.ds(pl.multiple_of(p * PAIR_KV, 128), PAIR_KV)
        wg_ref[:, at] = out * (1.0 / (2 * n_chips))

    @pl.loop(0, pairs + 3)
    def _(step):
        @pl.when(step + AHEAD < pairs)
        def _():
            start_sends(step + AHEAD)

        @pl.when(step >= 3)
        def _():
            stage_out(step - 3)

        @pl.when((step >= 2) & (step < pairs + 2))
        def _():
            stage_z(step - 2)

        @pl.when((step >= 1) & (step < pairs + 1))
        def _():
            stage_x(step - 1)

        @pl.when(step < pairs)
        def _():
            compute(step)

        @pl.when(step == pairs - 1)
        def _():
            for o in range(1, n_seq):
                at = pl.ds(pl.multiple_of(seq_to(o) * rows, rows), rows)
                lsend[o - 1] = lg_acc[at, :]
                send_l(o).start()

    own = lg_acc[pl.ds(pl.multiple_of(seq * rows, rows), rows), :]
    for o in range(1, n_seq):
        send_l(o).wait_recv()
        own = own + lrecv[o - 1]
    lg_ref[...] = own

    for o in range(1, n_seq):
        send_lat(o).wait_send()
        send_rope(o).wait_send()
        send_l(o).wait_send()

    @pl.loop(0, pairs)
    def _(p):
        for o in range(1, n_seq):
            send_q(p, o).wait_send()
            send_g(p, o).wait_send()
        send_d(p).wait_send()
        for o in range(1, nb):
            send_x(p, o).wait_send()
        for o in range(1, na):
            send_z(p, o).wait_send()


def per_device(queries, latent, key_rope, up_weight, out_grad):
    n_seq = lax.axis_size("seq")
    n_dp = lax.axis_size("dp")
    n_chips = n_dp // 2
    na = math.gcd(n_chips, 4)
    nb = n_chips // na
    rows, rank = latent.shape
    length = n_seq * rows
    pairs = up_weight.shape[1] // PAIR_KV
    block = rank // n_dp
    width = PAIR_KV
    dma = pltpu.SemaphoreType.DMA
    xs, zs, ss = max(nb - 1, 1), max(na - 1, 1), max(n_seq - 1, 1)
    return pl.pallas_call(
        functools.partial(kernel, n_seq, na, nb, pairs),
        out_shape=(
            jax.ShapeDtypeStruct((rows, rank), F32),
            jax.ShapeDtypeStruct((block, pairs * width), F32),
        ),
        in_specs=[pl.BlockSpec(memory_space=pl.ANY)] * 5,
        out_specs=[pl.BlockSpec(memory_space=pltpu.VMEM)] * 2,
        scratch_shapes=[
            pltpu.VMEM((pairs, n_seq, rows, PAIR_Q), BF16),
            pltpu.VMEM((pairs, n_seq, rows, PAIR_G), BF16),
            pltpu.VMEM((pairs, rank, width), BF16),
            pltpu.VMEM((n_seq, rows, rank), BF16),
            pltpu.VMEM((n_seq, rows, ROPE), BF16),
            pltpu.VMEM((rank, length), BF16),
            pltpu.VMEM((length, 128), F32),
            pltpu.VMEM((length, 128), F32),
            pltpu.VMEM((length, width), BF16),
            pltpu.VMEM((length, rank), F32),
            pltpu.VMEM((2, n_dp, block, width), F32),
            pltpu.VMEM((pairs, n_chips, block, width), BF16),
            pltpu.VMEM((pairs, n_chips, block, width), BF16),
            pltpu.VMEM((2, na, block, width), F32),
            pltpu.VMEM((pairs, xs, na, block, width), BF16),
            pltpu.VMEM((pairs, xs, na, block, width), BF16),
            pltpu.VMEM((2, block, width), F32),
            pltpu.VMEM((pairs, zs, block, width), BF16),
            pltpu.VMEM((pairs, zs, block, width), BF16),
            pltpu.VMEM((ss, rows, rank), F32),
            pltpu.VMEM((ss, rows, rank), F32),
            dma((pairs,)), dma((pairs,)), dma((pairs,)), dma, dma,
            dma((pairs, n_seq)), dma((pairs, n_seq)), dma((pairs, n_seq)), dma((pairs, n_seq)),
            dma((n_seq,)), dma((n_seq,)), dma((n_seq,)), dma((n_seq,)),
            dma((pairs,)), dma((pairs,)),
            dma((pairs, xs)), dma((pairs, xs)), dma((pairs, zs)), dma((pairs, zs)),
            dma((ss,)), dma((ss,)),
        ],
        compiler_params=pltpu.CompilerParams(
            collective_id=0, has_side_effects=True, vmem_limit_bytes=60 * 1024 * 1024
        ),
    )(queries, latent, key_rope, up_weight, out_grad)


def solution(mesh):
    placed = (
        P(("dp", "seq"), None),
        P(("dp", "seq"), None),
        P(("dp", "seq"), None),
        P(None, "seq"),
        P(("dp", "seq"), None),
    )
    return jax.shard_map(
        per_device,
        mesh=mesh,
        in_specs=placed,
        out_specs=(P(("dp", "seq"), None), P("dp", "seq")),
        check_vma=False,
    )
```

```python
import functools
import math

import jax
import jax.numpy as jnp
from jax import lax
from jax.experimental import pallas as pl
from jax.experimental.pallas import tpu as pltpu
from jax.sharding import PartitionSpec as P

NOPE = 128
ROPE = 64
VDIM = 128
QW = NOPE + ROPE
KVW = NOPE + VDIM
PAIR_Q = 2 * QW
PAIR_G = 2 * VDIM
PAIR_KV = 2 * KVW
AHEAD = 4
Z_LAG = 3
MESH = pl.DeviceIdType.MESH
F32 = jnp.float32
BF16 = jnp.bfloat16
NT = (((1,), (1,)), ((), ()))
TN = (((0,), (0,)), ((), ()))


def kernel(
    n_seq, na, nb, pairs,
    q_hbm, lat_hbm, rope_hbm, w_hbm, g_hbm,
    lg_ref, wg_ref,
    qbuf, gbuf, wbuf, latbuf, ropebuf, lat_t, rope_l, rope_r, keys, values, gc, lg_acc,
    part, dsend, drecv, keepx, xsend, xrecv, keepz, zsend, zrecv, lsend, lrecv,
    q_local, g_local, w_local, lat_local, rope_local,
    q_send, q_recv, g_send, g_recv, lat_send, lat_recv, rope_send, rope_recv,
    d_send, d_recv, x_send, x_recv, z_send, z_recv, l_send, l_recv,
):
    seq = lax.axis_index("seq")
    dp = lax.axis_index("dp")
    core = lax.rem(dp, 2)
    chip = dp // 2
    a_me = chip // nb
    b_me = lax.rem(chip, nb)
    n_chips = na * nb
    rows = lat_hbm.shape[0]
    length = n_seq * rows
    rank = lat_hbm.shape[1]
    block = rank // (2 * n_chips)
    scale = QW ** -0.5

    def seq_to(o):
        return lax.rem(seq + o, n_seq)

    def chip_core(a, b, c):
        return (a * nb + b) * 2 + c

    core_partner = chip_core(a_me, b_me, 1 - core)

    barrier = pltpu.get_barrier_semaphore()
    greeted = 0
    for o in range(1, n_seq):
        pl.semaphore_signal(barrier, inc=1, device_id={"seq": seq_to(o)}, device_id_type=MESH)
        greeted += 1
    pl.semaphore_signal(barrier, inc=1, device_id={"dp": core_partner}, device_id_type=MESH)
    greeted += 1
    for o in range(1, nb):
        pl.semaphore_signal(
            barrier, inc=1, device_id={"dp": chip_core(a_me, lax.rem(b_me + o, nb), core)},
            device_id_type=MESH,
        )
        greeted += 1
    for o in range(1, na):
        pl.semaphore_signal(
            barrier, inc=1, device_id={"dp": chip_core(lax.rem(a_me + o, na), b_me, core)},
            device_id_type=MESH,
        )
        greeted += 1

    def columns(owner, p, width):
        return pl.ds(pl.multiple_of((owner * pairs + p) * width, 128), width)

    def local_q(p):
        return pltpu.make_async_copy(
            q_hbm.at[:, columns(seq, p, PAIR_Q)], qbuf.at[p, seq], q_local.at[p]
        )

    def local_g(p):
        return pltpu.make_async_copy(
            g_hbm.at[:, columns(seq, p, PAIR_G)], gbuf.at[p, seq], g_local.at[p]
        )

    def local_w(p):
        return pltpu.make_async_copy(
            w_hbm.at[:, pl.ds(pl.multiple_of(p * PAIR_KV, 128), PAIR_KV)],
            wbuf.at[p], w_local.at[p],
        )

    local_lat = pltpu.make_async_copy(lat_hbm, latbuf.at[seq], lat_local)
    local_rope = pltpu.make_async_copy(rope_hbm, ropebuf.at[seq], rope_local)

    def remote(src, dst, send, recv, device):
        return pltpu.make_async_remote_copy(
            src_ref=src, dst_ref=dst, send_sem=send, recv_sem=recv,
            device_id=device, device_id_type=MESH,
        )

    def send_lat(o):
        return remote(lat_hbm, latbuf.at[seq], lat_send.at[o], lat_recv.at[o], {"seq": seq_to(o)})

    def send_rope(o):
        return remote(
            rope_hbm, ropebuf.at[seq], rope_send.at[o], rope_recv.at[o], {"seq": seq_to(o)}
        )

    def send_q(p, o):
        return remote(
            q_hbm.at[:, columns(seq_to(o), p, PAIR_Q)], qbuf.at[p, seq],
            q_send.at[p, o], q_recv.at[p, o], {"seq": seq_to(o)},
        )

    def send_g(p, o):
        return remote(
            g_hbm.at[:, columns(seq_to(o), p, PAIR_G)], gbuf.at[p, seq],
            g_send.at[p, o], g_recv.at[p, o], {"seq": seq_to(o)},
        )

    def send_d(p):
        return remote(dsend.at[p], drecv.at[p], d_send.at[p], d_recv.at[p], {"dp": core_partner})

    def send_x(p, o):
        return remote(
            xsend.at[p, o - 1], xrecv.at[p, o - 1], x_send.at[p, o - 1], x_recv.at[p, o - 1],
            {"dp": chip_core(a_me, lax.rem(b_me + o, nb), core)},
        )

    def send_z(p, o):
        return remote(
            zsend.at[p, o - 1], zrecv.at[p, o - 1], z_send.at[p, o - 1], z_recv.at[p, o - 1],
            {"dp": chip_core(lax.rem(a_me + o, na), b_me, core)},
        )

    def send_l(o):
        return remote(
            lsend.at[o - 1], lrecv.at[o - 1], l_send.at[o - 1], l_recv.at[o - 1],
            {"seq": seq_to(o)},
        )

    local_lat.start()
    local_rope.start()

    @pl.loop(0, pairs)
    def _(p):
        local_w(p).start()
        local_q(p).start()
        local_g(p).start()

    pl.semaphore_wait(barrier, greeted)

    for o in range(1, n_seq):
        send_lat(o).start()
        send_rope(o).start()

    def start_sends(p):
        for o in range(1, n_seq):
            send_q(p, o).start()
            send_g(p, o).start()

    @pl.loop(0, min(AHEAD, pairs))
    def _(p):
        start_sends(p)

    local_lat.wait()
    local_rope.wait()
    for o in range(1, n_seq):
        send_lat(o).wait_recv()
        send_rope(o).wait_recv()

    for s in range(n_seq):
        lat_t[:, s * rows:(s + 1) * rows] = latbuf[s].T
        rope = ropebuf[s]
        from_lane = lax.broadcasted_iota(jnp.int32, (ROPE, 128), 0)
        to_lane = lax.broadcasted_iota(jnp.int32, (ROPE, 128), 1)
        low = (from_lane == to_lane).astype(F32).astype(BF16)
        high = (from_lane + (128 - ROPE) == to_lane).astype(F32).astype(BF16)
        rope_l[s * rows:(s + 1) * rows] = lax.dot_general(rope, low, TN, preferred_element_type=F32)
        rope_r[s * rows:(s + 1) * rows] = lax.dot_general(rope, high, TN, preferred_element_type=F32)
    lg_acc[...] = jnp.zeros_like(lg_acc)

    span = math.gcd(length, 256)
    n_blocks = length // span
    lane = lax.broadcasted_iota(jnp.int32, (length, 128), 1)
    lower = lane < 64

    def head(head_keys, head_values, q_all, g_all):
        key_parts = [None] * n_blocks
        value_parts = [None] * n_blocks
        for b in range(n_blocks):
            end = (b + 1) * span
            q = q_all[b * span:end]
            g = g_all[b * span:end]
            scores = lax.dot_general(head_keys[:end], q, NT, preferred_element_type=F32) * scale
            key_pos = lax.broadcasted_iota(jnp.int32, (end, span), 0)
            query_pos = b * span + lax.broadcasted_iota(jnp.int32, (end, span), 1)
            scores = jnp.where(key_pos <= query_pos, scores, F32(-1e30))
            top = jnp.max(scores, axis=0, keepdims=True)
            expo = jnp.exp(scores - top)
            probs = expo * (1.0 / jnp.sum(expo, axis=0, keepdims=True))
            value_part = jnp.dot(probs.astype(BF16), g, preferred_element_type=F32)
            prob_grad = lax.dot_general(head_values[:end], g, NT, preferred_element_type=F32)
            row_dot = jnp.sum(probs * prob_grad, axis=0, keepdims=True)
            score_grad = (probs * (prob_grad - row_dot) * scale).astype(BF16)
            key_part = jnp.dot(score_grad, q, preferred_element_type=F32)
            for k in range(b + 1):
                at = slice(k * span, (k + 1) * span)
                if key_parts[k] is None:
                    key_parts[k], value_parts[k] = key_part[at], value_part[at]
                else:
                    key_parts[k] = key_parts[k] + key_part[at]
                    value_parts[k] = value_parts[k] + value_part[at]
        if n_blocks == 1:
            return key_parts[0], value_parts[0]
        return jnp.concatenate(key_parts, axis=0), jnp.concatenate(value_parts, axis=0)

    def make_keys(p):
        lat = latbuf[...].reshape(length, rank)
        local_w(p).wait()
        kv = jnp.dot(lat, wbuf[p], preferred_element_type=F32)
        keys[0] = jnp.concatenate([kv[:, :128], rope_l[...]], axis=1).astype(BF16)
        turned = pltpu.roll(kv[:, 256:384], 64, 1)
        keys[1] = jnp.concatenate(
            [jnp.where(lower, 0.0, turned), jnp.where(lower, turned, rope_r[...])], axis=1
        ).astype(BF16)
        values[0] = kv[:, 128:256].astype(BF16)
        values[1] = kv[:, 384:512].astype(BF16)

    def compute(p):
        local_q(p).wait()
        local_g(p).wait()
        for o in range(1, n_seq):
            send_q(p, o).wait_recv()
            send_g(p, o).wait_recv()
        q_all = qbuf[p].reshape(length, PAIR_Q)
        g_all = gbuf[p].reshape(length, PAIR_G)
        kg0, vg0 = head(keys[0], values[0], q_all[:, :256], g_all[:, :128])
        gc[:, 0:128] = kg0[:, :128].astype(BF16)
        gc[:, 128:256] = vg0.astype(BF16)
        kg1, vg1 = head(keys[1], values[1], q_all[:, 128:384], g_all[:, 128:])
        kg1 = jnp.where(lower, pltpu.roll(kg1[:, :128], 64, 1), pltpu.roll(kg1[:, 128:], 64, 1))
        gc[:, 256:384] = kg1.astype(BF16)
        gc[:, 384:512] = vg1.astype(BF16)
        grads = gc[...]
        slot = lax.rem(p, 2)
        product = jnp.dot(lat_t[...], grads, preferred_element_type=F32)
        for d in range(2 * n_chips):
            part[slot, d] = product[d * block:(d + 1) * block]
        for k in range(n_chips):
            dsend[p, k] = part[slot, 2 * k + 1 - core].astype(BF16)
        send_d(p).start()
        lg_acc[...] += lax.dot_general(grads, wbuf[p], NT, preferred_element_type=F32)

    def stage_x(p):
        slot = lax.rem(p, 2)
        send_d(p).wait_recv()

        def chip_sum(k):
            return part[slot, 2 * k + core] + drecv[p, k].astype(F32)

        for o in range(1, nb):
            b = lax.rem(b_me + o, nb)
            for a in range(na):
                xsend[p, o - 1, a] = chip_sum(a * nb + b).astype(BF16)
            send_x(p, o).start()
        for a in range(na):
            keepx[p, a] = chip_sum(a * nb + b_me)

    def stage_z(p):
        for o in range(1, nb):
            send_x(p, o).wait_recv()

        def total(a):
            out = keepx[p, a]
            for o in range(1, nb):
                out = out + xrecv[p, o - 1, a].astype(F32)
            return out

        for o in range(1, na):
            zsend[p, o - 1] = total(lax.rem(a_me + o, na)).astype(BF16)
            send_z(p, o).start()
        keepz[p] = total(a_me)

    def stage_out(p):
        out = keepz[p]
        for o in range(1, na):
            send_z(p, o).wait_recv()
            out = out + zrecv[p, o - 1].astype(F32)
        at = pl.ds(pl.multiple_of(p * PAIR_KV, 128), PAIR_KV)
        wg_ref[:, at] = out * (1.0 / (2 * n_chips))

    @pl.loop(0, pairs + Z_LAG)
    def _(step):
        @pl.when(step + AHEAD < pairs)
        def _():
            start_sends(step + AHEAD)

        @pl.when(step < pairs)
        def _():
            make_keys(step)

        @pl.when((step >= 1) & (step < pairs + 1))
        def _():
            stage_x(step - 1)

        @pl.when(step >= Z_LAG)
        def _():
            stage_z(step - Z_LAG)

        @pl.when(step < pairs)
        def _():
            compute(step)

        @pl.when(step == pairs - 1)
        def _():
            for o in range(1, n_seq):
                at = pl.ds(pl.multiple_of(seq_to(o) * rows, rows), rows)
                lsend[o - 1] = lg_acc[at, :]
                send_l(o).start()

    own = lg_acc[pl.ds(pl.multiple_of(seq * rows, rows), rows), :]
    for o in range(1, n_seq):
        send_l(o).wait_recv()
        own = own + lrecv[o - 1]
    lg_ref[...] = own

    @pl.loop(0, pairs)
    def _(p):
        stage_out(p)

    for o in range(1, n_seq):
        send_lat(o).wait_send()
        send_rope(o).wait_send()
        send_l(o).wait_send()

    @pl.loop(0, pairs)
    def _(p):
        for o in range(1, n_seq):
            send_q(p, o).wait_send()
            send_g(p, o).wait_send()
        send_d(p).wait_send()
        for o in range(1, nb):
            send_x(p, o).wait_send()
        for o in range(1, na):
            send_z(p, o).wait_send()


def per_device(queries, latent, key_rope, up_weight, out_grad):
    n_seq = lax.axis_size("seq")
    n_dp = lax.axis_size("dp")
    n_chips = n_dp // 2
    na = math.gcd(n_chips, 4)
    nb = n_chips // na
    rows, rank = latent.shape
    length = n_seq * rows
    pairs = up_weight.shape[1] // PAIR_KV
    block = rank // n_dp
    width = PAIR_KV
    dma = pltpu.SemaphoreType.DMA
    xs, zs, ss = max(nb - 1, 1), max(na - 1, 1), max(n_seq - 1, 1)
    results = pl.pallas_call(
        functools.partial(kernel, n_seq, na, nb, pairs),
        out_shape=(
            jax.ShapeDtypeStruct((rows, rank), F32),
            jax.ShapeDtypeStruct((block, pairs * width), F32),
        ),
        in_specs=[pl.BlockSpec(memory_space=pl.ANY)] * 5,
        out_specs=[pl.BlockSpec(memory_space=pltpu.VMEM)] * 2,
        scratch_shapes=[
            pltpu.VMEM((pairs, n_seq, rows, PAIR_Q), BF16),
            pltpu.VMEM((pairs, n_seq, rows, PAIR_G), BF16),
            pltpu.VMEM((pairs, rank, width), BF16),
            pltpu.VMEM((n_seq, rows, rank), BF16),
            pltpu.VMEM((n_seq, ROPE, rows), BF16),
            pltpu.VMEM((rank, length), BF16),
            pltpu.VMEM((length, 128), F32),
            pltpu.VMEM((length, 128), F32),
            pltpu.VMEM((2, length, 256), BF16),
            pltpu.VMEM((2, length, 128), BF16),
            pltpu.VMEM((length, width), BF16),
            pltpu.VMEM((length, rank), F32),
            pltpu.VMEM((2, n_dp, block, width), F32),
            pltpu.VMEM((pairs, n_chips, block, width), BF16),
            pltpu.VMEM((pairs, n_chips, block, width), BF16),
            pltpu.VMEM((pairs, na, block, width), F32),
            pltpu.VMEM((pairs, xs, na, block, width), BF16),
            pltpu.VMEM((pairs, xs, na, block, width), BF16),
            pltpu.VMEM((pairs, block, width), F32),
            pltpu.VMEM((pairs, zs, block, width), BF16),
            pltpu.VMEM((pairs, zs, block, width), BF16),
            pltpu.VMEM((ss, rows, rank), F32),
            pltpu.VMEM((ss, rows, rank), F32),
            dma((pairs,)), dma((pairs,)), dma((pairs,)), dma, dma,
            dma((pairs, n_seq)), dma((pairs, n_seq)), dma((pairs, n_seq)), dma((pairs, n_seq)),
            dma((n_seq,)), dma((n_seq,)), dma((n_seq,)), dma((n_seq,)),
            dma((pairs,)), dma((pairs,)),
            dma((pairs, xs)), dma((pairs, xs)), dma((pairs, zs)), dma((pairs, zs)),
            dma((ss,)), dma((ss,)),
        ],
        compiler_params=pltpu.CompilerParams(
            collective_id=0, has_side_effects=True, vmem_limit_bytes=60 * 1024 * 1024
        ),
    )(queries, latent, key_rope.T, up_weight, out_grad)
    return pl.pallas_call(
        put_out,
        out_shape=tuple(jax.ShapeDtypeStruct(r.shape, r.dtype) for r in results),
        in_specs=[pl.BlockSpec(memory_space=pltpu.VMEM)] * 2,
        out_specs=[pl.BlockSpec(memory_space=pl.ANY)] * 2,
        scratch_shapes=[pltpu.SemaphoreType.DMA((2,))],
    )(*results)


def put_out(lg_in, wg_in, lg_out, wg_out, sems):
    copies = (
        pltpu.make_async_copy(lg_in, lg_out, sems.at[0]),
        pltpu.make_async_copy(wg_in, wg_out, sems.at[1]),
    )
    for copy in copies:
        copy.start()
    for copy in copies:
        copy.wait()


def solution(mesh):
    placed = (
        P(("dp", "seq"), None),
        P(("dp", "seq"), None),
        P(("dp", "seq"), None),
        P(None, "seq"),
        P(("dp", "seq"), None),
    )
    return jax.shard_map(
        per_device,
        mesh=mesh,
        in_specs=placed,
        out_specs=(P(("dp", "seq"), None), P("dp", "seq")),
        check_vma=False,
    )
```
